32 devices in a mesh: groups: 1, ep: 8 (over z, y), tp: 2 (over x), sub: 2 (over core).
Axes of the slice: x: 2, y: 2, z: 4, core: 2. Of those that a mesh axis runs over, the one named last changes fastest.
Arguments:
- queries: bfloat16 [128, 64, 128], P(('groups', 'ep', 'sub'), 'tp'), may hold values from -80 to 80
- new_keys: bfloat16 [128, 4, 128], P(('groups', 'ep', 'sub'), 'tp'), may hold values from -4 to 4
- new_values: bfloat16 [128, 4, 128], P(('groups', 'ep', 'sub'), 'tp'), may hold values from -5 to 5
- key_codes: int32 [128, 4, 8, 128], P(('groups', 'ep', 'sub'), 'tp'), may hold values from -2147483648 to 2147483647, as said below
- key_scale: bfloat16 [128, 4, 4, 128], P(('groups', 'ep', 'sub'), 'tp'), may hold values from 0.19921875 to 1
- key_zero: bfloat16 [128, 4, 4, 128], P(('groups', 'ep', 'sub'), 'tp'), may hold values from -1.5 to 0.5
- value_codes: int32 [128, 4, 8, 128], P(('groups', 'ep', 'sub'), 'tp'), may hold values from -2147483648 to 2147483647, as said below
- value_scale: bfloat16 [128, 4, 128], P(('groups', 'ep', 'sub'), 'tp'), may hold values from 0.19921875 to 1
- value_zero: bfloat16 [128, 4, 128], P(('groups', 'ep', 'sub'), 'tp'), may hold values from -1.1953125 to 0.19921875
- lengths: int32 [128], P(('groups', 'ep', 'sub')), may hold values from 1 to 128, as said below
- out_weight: bfloat16 [8192, 2048], P('tp', ('ep', 'sub')), may hold values from -0.0625 to 0.0625
- residual: bfloat16 [128, 2048], P(('groups', 'ep', 'sub'), 'tp'), may hold values from -8 to 8
- norm_gain: bfloat16 [2048], P('tp'), may hold values from 0.099609375 to 1.8984375
- expert_ids: int32 [128, 8], P(('groups', 'ep', 'sub')), may hold values from 0 to 15, all different within a row; in each aligned block of 8 rows (0 to 7, 8 to 15, ...) at most 8 rows name the same one
- route_weights: int32 [128, 8], P(('groups', 'ep', 'sub')), may hold values from 1 to 65535
- capacity: int32 [16], P('groups'), may hold values from 16 to 32, as said below
- w_gate: bfloat16 [16, 2048, 768], P(('ep', 'sub'), 'tp'), may hold values from -0.125 to 0.125
- w_up: bfloat16 [16, 2048, 768], P(('ep', 'sub'), 'tp'), may hold values from -0.125 to 0.125
- w_down: bfloat16 [16, 768, 2048], P(('ep', 'sub'), None, 'tp'), may hold values from -0.21875 to 0.21875
Outputs:
- mixed: bfloat16 [128, 2048], P(('groups', 'ep', 'sub'), 'tp')
The draws below stay inside these ranges and needn't reach their ends.
Inputs may be any that keep to these rules, and one draw needn't show every extreme that they name: `key_codes`: each word holds 16 two-bit codes: position 16 w + j in bits 2 j and 2 j + 1 of word w. `value_codes`: packed as key_codes. `lengths`: some request of the batch has exactly 128 cached positions. `expert_ids`: each row names 8 different experts; within the rows of one device (aligned blocks of 8 rows) no expert is named by more than 8 rows, and that bound is reached. Several experts have capacity 32.
All inputs are finite; a program needn't handle non-finite values.
Results may differ from the reference program's by a relative error of at most 0.014.
Values may be sent and summed in bfloat16 or wider, within the bound.
A program may use at most 64 MiB of HBM per device.

```python
import math
import jax
import jax.numpy as jnp
import numpy as np
from jax import lax

D = 2048
FF = 768
HQ = 64
KV = 4
HD = 128
TOP = 8
GROUP = 32
REQ = 8
LMAX = 128
BATCH = 128
EXPERTS = 16
SLOT = 8
CAP = 32


def fresh_keys(key):
    drawn = jax.random.normal(jax.random.fold_in(key, 11), (BATCH, KV, HD), jnp.float32)
    return jnp.clip(drawn, -4.0, 4.0)


def draw_new_keys(key, part):
    return fresh_keys(key).astype(jnp.bfloat16)


def draw_queries(key, part):
    drawn = jnp.clip(jax.random.normal(jax.random.fold_in(key, 12), (BATCH, HQ, HD), jnp.float32), -5.0, 5.0)
    return drawn.astype(jnp.bfloat16)


def packed_codes(key):
    word_shape = (BATCH, KV, LMAX // 16, HD)
    high_half = jax.random.randint(jax.random.fold_in(key, 1), word_shape, 0, 65536, jnp.int32)
    low_half = jax.random.randint(jax.random.fold_in(key, 2), word_shape, 0, 65536, jnp.int32)
    return jnp.bitwise_or(jnp.left_shift(high_half, jnp.int32(16)), low_half).astype(jnp.int32)


def draw_key_codes(key, part):
    return packed_codes(jax.random.fold_in(key, 21))


def draw_value_codes(key, part):
    return packed_codes(jax.random.fold_in(key, 22))


def draw_lengths(key, part):
    drawn = jax.random.randint(jax.random.fold_in(key, 31), (BATCH,), 1, LMAX + 1, jnp.int32)
    full_row = jax.random.randint(jax.random.fold_in(key, 32), (), 0, BATCH, jnp.int32)
    return jnp.where(jnp.arange(BATCH) == full_row, LMAX, drawn).astype(jnp.int32)


def draw_capacity(key, part):
    drawn = jax.random.randint(jax.random.fold_in(key, 51), (EXPERTS,), CAP // 2, CAP + 1, jnp.int32)
    at_most = jax.random.randint(jax.random.fold_in(key, 52), (EXPERTS,), 0, 4, jnp.int32) == 0
    full_one = jax.random.randint(jax.random.fold_in(key, 53), (), 0, EXPERTS, jnp.int32)
    at_most = at_most | (jnp.arange(EXPERTS) == full_one)
    return jnp.where(at_most, CAP, drawn).astype(jnp.int32)


def draw_residual(key, part):
    drawn = 0.5 * jax.random.normal(jax.random.fold_in(key, 41), (BATCH, D), jnp.float32)
    return jnp.clip(drawn, -8.0, 8.0).astype(jnp.bfloat16)


def set_ends(values, stream_key, smallest, largest):
    place = [jax.random.randint(jax.random.fold_in(stream_key, axis), (), 0, length) for axis, length in enumerate(values.shape)]
    longest = values.shape.index(max(values.shape))
    next_to = place[:longest] + [(place[longest] + 1) % values.shape[longest]] + place[longest + 1:]
    return values.at[tuple(place)].set(smallest).at[tuple(next_to)].set(largest)


def block_scale(key, extent, shards, low, top_value):
    gain, own = 1.0, jax.random.fold_in(key, 6)
    for axis_at, blocks in shards:
        steps = jnp.exp(jax.random.uniform(jax.random.fold_in(own, axis_at), (blocks,), jnp.float32, low / len(shards), top_value / len(shards)))
        gain = gain * jnp.repeat(steps, extent[axis_at] // blocks).reshape([-1 if axis == axis_at else 1 for axis in range(len(extent))])
    return gain


def routed_block(own_key, own, number, rows, number_of, top, reach, skew):
    order = jax.random.permutation(own_key, number_of)
    crowded, ordinary = load_shares(number_of, rows * top, reach, skew, True), load_shares(number_of, rows * top, reach, skew, False)
    places = jnp.arange(number_of)

    def named(sizes, offset_by):
        used = int((sizes > 0).sum())
        fixed = max(1, used // 4)
        shifted = fixed + (places - fixed + offset_by * (used - fixed)) % max(1, number_of - fixed)
        return jnp.zeros((number_of,), jnp.int32).at[order[jnp.where(places < fixed, places, shifted)]].set(jnp.asarray(sizes, jnp.int32))

    sizes = jnp.where(number % 4 == 0, named(crowded, number // 4), named(ordinary, number - number // 4 - 1))
    mixed = jax.random.permutation(jax.random.fold_in(own, 3), number_of)
    donor, sink = mixed[0:number_of // 2 * 2:2], mixed[1:number_of // 2 * 2:2]
    slack = jnp.minimum(sizes[donor] - 1, reach - sizes[sink]) // 2
    slack = jnp.where((donor == order[0]) | (sink == order[0]) | (sizes[sink] == 0), 0, jnp.maximum(slack, 0))
    shifted = jax.random.randint(jax.random.fold_in(own, 4), (number_of // 2,), 0, 1 << 20) % (slack + 1)
    sizes = sizes.at[donor].add(-shifted).at[sink].add(shifted)
    items = jnp.searchsorted(jnp.cumsum(sizes), jnp.arange(rows * top), side="right").astype(jnp.int32)
    grid = items.reshape(top, rows).T
    grid = grid[jax.random.permutation(jax.random.fold_in(own, 1), rows)]
    offset_by = jax.random.randint(jax.random.fold_in(own, 2), (rows, 1), 0, top)
    return jnp.take_along_axis(grid, (jnp.arange(top)[None, :] + offset_by) % top, axis=1)


def load_shares(amount, total, limit, skew, full):
    portions = [(1 << 20) // math.isqrt(standing ** skew) + 1 for standing in range(1, amount + 1)]
    largest = limit if full else min(limit, max(-(-total // amount), total * portions[0] // sum(portions)))
    least = 1 if total - largest >= amount - 1 else 0
    given, surplus = [largest] + [least] * (amount - 1), total - largest - least * (amount - 1)
    while surplus > 0:
        candidates = [i for i in range(1, amount) if given[i] < largest] or [i for i in range(1, amount) if given[i] < limit]
        whole, budget = sum([portions[i] for i in candidates]), surplus
        for i in candidates:
            extra = min(limit - given[i], max(1, budget * portions[i] // whole), surplus)
            given[i] = given[i] + extra
            surplus = surplus - extra
    return np.array(given)


def normal_values(rng, dims, spread, reach, shards=(), held_as=jnp.bfloat16):
    gain = block_scale(rng, dims, shards, -0.22, 0.18) if shards else 1.0
    values = jax.random.normal(rng, dims, jnp.float32) * spread * gain
    return jnp.minimum(jnp.maximum(values, -reach), reach).astype(held_as)


def setup_inputs(seed: int = 0, part: int = 0) -> dict:
    key_of = jax.random.split(jax.random.key(seed), 20)
    own_keys = jax.random.split(jax.random.fold_in(key_of[19], part), 20)
    queries = draw_queries(jax.random.fold_in(jax.random.fold_in(key_of[19], part), 71), part)
    new_keys = draw_new_keys(jax.random.fold_in(jax.random.fold_in(key_of[19], part), 71), part)
    new_values = normal_values(own_keys[2], (BATCH, KV, HD), 1.0, 5.0, ((0, 16), (1, 2)))
    key_codes = draw_key_codes(jax.random.fold_in(jax.random.fold_in(key_of[19], part), 71), part)
    key_scale = jnp.clip(0.19921875 + 0.80078125 * jax.random.uniform(own_keys[4], (BATCH, KV, LMAX // GROUP, HD), jnp.float32) ** block_scale(own_keys[4], (BATCH, KV, LMAX // GROUP, HD), ((0, 16), (1, 2)), -0.2, 0.2), 0.19921875, 1.0).astype(jnp.bfloat16)
    key_zero = jnp.clip(-1.5 + 2.0 * jax.random.uniform(own_keys[5], (BATCH, KV, LMAX // GROUP, HD), jnp.float32) ** block_scale(own_keys[5], (BATCH, KV, LMAX // GROUP, HD), ((0, 16), (1, 2)), -0.2, 0.2), -1.5, 0.5).astype(jnp.bfloat16)
    value_codes = draw_value_codes(jax.random.fold_in(jax.random.fold_in(key_of[19], part), 71), part)
    value_scale = jnp.clip(0.19921875 + 0.80078125 * jax.random.uniform(own_keys[7], (BATCH, KV, LMAX), jnp.float32) ** block_scale(own_keys[7], (BATCH, KV, LMAX), ((0, 16), (1, 2)), -0.2, 0.2), 0.19921875, 1.0).astype(jnp.bfloat16)
    value_zero = jnp.clip(-1.1953125 + 1.3945312 * jax.random.uniform(own_keys[8], (BATCH, KV, LMAX), jnp.float32) ** block_scale(own_keys[8], (BATCH, KV, LMAX), ((0, 16), (1, 2)), -0.2, 0.2), -1.1953125, 0.19921875).astype(jnp.bfloat16)
    lengths = draw_lengths(jax.random.fold_in(jax.random.fold_in(key_of[19], part), 71), part)
    out_weight = normal_values(key_of[10], (HQ * HD, D), (HQ * HD) ** -0.5, 0.0625, ((0, 2), (1, 16)))
    residual = draw_residual(jax.random.fold_in(jax.random.fold_in(key_of[19], part), 71), part)
    norm_gain = jnp.clip(1.0 + 0.18 * jax.random.normal(key_of[12], (D,), jnp.float32), 0.099609375, 1.8984375).astype(jnp.bfloat16)
    expert_ids_keys = jax.random.split(jax.random.fold_in(own_keys[13], 1), BATCH // REQ)
    expert_ids_turns = jax.random.permutation(jax.random.fold_in(own_keys[13], 3), BATCH // REQ)
    expert_ids = jax.vmap(lambda own, number: routed_block(jax.random.fold_in(own_keys[13], 2), own, number, REQ, EXPERTS, TOP, SLOT, 2))(expert_ids_keys, expert_ids_turns).reshape((BATCH, TOP))
    route_weights = set_ends(jax.random.randint(own_keys[14], (BATCH, TOP), 1, 65536), jax.random.fold_in(own_keys[14], 1), 1, 65535).astype(jnp.int32)
    capacity = draw_capacity(jax.random.fold_in(jax.random.fold_in(key_of[19], part), 71), part)
    w_gate = normal_values(key_of[16], (EXPERTS, D, FF), D ** -0.5, 0.125, ((0, 16), (1, 2)))
    w_up = normal_values(key_of[17], (EXPERTS, D, FF), D ** -0.5, 0.125, ((0, 16), (1, 2)))
    w_down = normal_values(key_of[18], (EXPERTS, FF, D), FF ** -0.5, 0.21875, ((0, 16), (2, 2)))
    return {"queries": queries, "new_keys": new_keys, "new_values": new_values, "key_codes": key_codes, "key_scale": key_scale, "key_zero": key_zero, "value_codes": value_codes, "value_scale": value_scale, "value_zero": value_zero, "lengths": lengths, "out_weight": out_weight, "residual": residual, "norm_gain": norm_gain, "expert_ids": expert_ids, "route_weights": route_weights, "capacity": capacity, "w_gate": w_gate, "w_up": w_up, "w_down": w_down}


EPS = 1e-06

def unpack_codes(packed_words):
    shifts = (2 * jnp.arange(16)).astype(jnp.int32)
    code_vals = jnp.bitwise_and(jnp.right_shift(packed_words[..., None, :], shifts[:, None]), 3)
    word_shape = packed_words.shape
    return code_vals.reshape(word_shape[:-2] + (word_shape[-2] * 16, word_shape[-1])).astype(jnp.float32)

def attend_one(request_data):
    query_heads, key_new, value_new, key_words, key_step, key_offset, value_words, value_step, value_offset, seq_length = request_data
    kv_heads, head_dim = key_new.shape
    token_group = key_words.shape[1] * 16 // key_step.shape[1]
    keys_deq = unpack_codes(key_words) * jnp.repeat(key_step.astype(jnp.float32), token_group, axis=1)
    keys_deq = (keys_deq + jnp.repeat(key_offset.astype(jnp.float32), token_group, axis=1)).astype(jnp.bfloat16)
    values_deq = unpack_codes(value_words) * value_step.astype(jnp.float32)[:, :, None] + value_offset.astype(jnp.float32)[:, :, None]
    values_deq = values_deq.astype(jnp.bfloat16)
    grouped = query_heads.reshape(kv_heads, -1, head_dim).astype(jnp.float32)
    inv_scale = 1.0 / math.sqrt(head_dim)
    scores = jnp.einsum('kgd,kld->kgl', grouped, keys_deq.astype(jnp.float32)) * inv_scale
    own_score = jnp.einsum('kgd,kd->kg', grouped, key_new.astype(jnp.float32)) * inv_scale
    usable = jnp.arange(keys_deq.shape[1]) < seq_length
    scores = jnp.where(usable, scores, -jnp.inf)
    highest = jnp.maximum(lax.optimization_barrier(jnp.max(scores, axis=2)), own_score)
    weights = jnp.exp(scores - highest[:, :, None])
    own_weight = jnp.exp(own_score - highest)
    totals = lax.optimization_barrier(jnp.sum(weights, axis=2)) + own_weight
    weights = (weights / totals[:, :, None]).astype(jnp.bfloat16)
    own_weight = (own_weight / totals).astype(jnp.bfloat16)
    result = jnp.einsum('kgl,kld->kgd', weights.astype(jnp.float32), values_deq.astype(jnp.float32))
    result = result + own_weight.astype(jnp.float32)[:, :, None] * value_new.astype(jnp.float32)[:, None, :]
    return result.reshape(-1).astype(jnp.bfloat16)

def reference(queries, new_keys, new_values, key_codes, key_scale, key_zero, value_codes, value_scale, value_zero, lengths, out_weight, residual, norm_gain, expert_ids, route_weights, capacity, w_gate, w_up, w_down):
    attended = lax.map(attend_one, (queries, new_keys, new_values, key_codes, key_scale, key_zero, value_codes, value_scale, value_zero, lengths))
    projected = jnp.dot(attended, out_weight, preferred_element_type=jnp.float32)
    hidden_state = residual.astype(jnp.float32) + projected
    mean_square = lax.optimization_barrier(jnp.mean(hidden_state * hidden_state, axis=1, keepdims=True))
    normed = (hidden_state * lax.rsqrt(mean_square + EPS) * norm_gain.astype(jnp.float32)).astype(jnp.bfloat16)
    raw_weight = route_weights.astype(jnp.float32)
    shares = raw_weight / lax.optimization_barrier(jnp.sum(raw_weight, axis=1, keepdims=True))
    experts_all = w_gate.shape[0]
    chosen = (expert_ids[:, :, None] == jnp.arange(experts_all).astype(jnp.int32)).astype(jnp.int32)
    is_named = lax.optimization_barrier(jnp.sum(chosen, axis=1)).astype(jnp.int32)
    rank = (jnp.cumsum(is_named, axis=0) - is_named).astype(jnp.int32)
    kept = is_named * (rank < capacity[None, :]).astype(jnp.int32)
    weight_per = lax.optimization_barrier(jnp.sum(chosen.astype(jnp.float32) * shares[:, :, None], axis=1)) * kept.astype(jnp.float32)
    slot_ids = jnp.arange(CAP).astype(jnp.int32)

    def one_expert(totals, per_expert):
        keep_col, rank_col, weight_col, gate_w, up_w, down_w = per_expert
        packer = ((rank_col[None, :] == slot_ids[:, None]) & (keep_col[None, :] > 0)).astype(jnp.bfloat16)
        packed_rows = jnp.dot(packer, normed, preferred_element_type=jnp.float32).astype(jnp.bfloat16)
        gate_sum = jnp.dot(packed_rows, gate_w, preferred_element_type=jnp.float32)
        up_sum = jnp.dot(packed_rows, up_w, preferred_element_type=jnp.float32)
        activated = (jax.nn.silu(gate_sum) * up_sum).astype(jnp.bfloat16)
        expert_out = jnp.dot(activated, down_w, preferred_element_type=jnp.float32).astype(jnp.bfloat16)
        spread_back = jnp.dot(packer.T, expert_out, preferred_element_type=jnp.float32)
        return (totals + weight_col[:, None] * spread_back, None)
    moe, _ = lax.scan(one_expert, jnp.zeros(hidden_state.shape, jnp.float32), (kept.T, rank.T, weight_per.T, w_gate, w_up, w_down))
    return (hidden_state + moe).astype(jnp.bfloat16)
```

```python
import functools
import math

import jax
import jax.numpy as jnp
from jax import lax
from jax.experimental import pallas as pl
from jax.experimental.pallas import tpu as pltpu
from jax.sharding import PartitionSpec as P

EPS = 1e-06


def carried_in(value, axis, join, neutral):
    count, mine = (lax.axis_size(axis), lax.axis_index(axis))
    pieces = lax.all_gather(value, axis)
    total = jnp.full_like(value, 0) + jnp.asarray(neutral, value.dtype)

    def turn(position, total):
        longer = join(total, pieces[position])
        return jnp.where(position < mine, longer, total)

    return lax.fori_loop(0, count - 1, turn, total)


def unpack_codes(packed_words):
    shifts = 2 * jnp.arange(16)
    code_vals = jnp.bitwise_and(jnp.right_shift(packed_words[..., None, :], shifts[:, None]), 3)
    word_shape = packed_words.shape
    return code_vals.reshape(word_shape[:-2] + (word_shape[-2] * 16, word_shape[-1])).astype(
        jnp.float32
    )


def attend_one(request_data):
    (
        query_heads,
        key_new,
        value_new,
        key_words,
        key_step,
        key_offset,
        value_words,
        value_step,
        value_offset,
        seq_length,
    ) = request_data
    kv_heads, head_dim = key_new.shape
    token_group = key_words.shape[1] * 16 // key_step.shape[1]
    keys_deq = unpack_codes(key_words) * jnp.repeat(
        key_step.astype(jnp.float32), token_group, axis=1
    )
    keys_deq = (keys_deq + jnp.repeat(key_offset.astype(jnp.float32), token_group, axis=1)).astype(
        jnp.bfloat16
    )
    values_deq = (
        unpack_codes(value_words) * value_step.astype(jnp.float32)[:, :, None]
        + value_offset.astype(jnp.float32)[:, :, None]
    )
    values_deq = values_deq.astype(jnp.bfloat16)
    grouped = query_heads.reshape(kv_heads, -1, head_dim)
    inv_scale = 1.0 / math.sqrt(head_dim)
    scores = (
        jnp.einsum("kgd,kld->kgl", grouped, keys_deq, preferred_element_type=jnp.float32)
        * inv_scale
    )
    own_score = (
        jnp.einsum("kgd,kd->kg", grouped, key_new, preferred_element_type=jnp.float32) * inv_scale
    )
    usable = jnp.arange(keys_deq.shape[1]) < seq_length
    scores = jnp.where(usable, scores, -jnp.inf)
    highest = jnp.maximum(jnp.max(scores, axis=2), own_score)
    weights = jnp.exp(scores - highest[:, :, None])
    own_weight = jnp.exp(own_score - highest)
    totals = jnp.sum(weights, axis=2) + own_weight
    weights = (weights / totals[:, :, None]).astype(jnp.bfloat16)
    own_weight = (own_weight / totals).astype(jnp.bfloat16)
    result = jnp.einsum("kgl,kld->kgd", weights, values_deq, preferred_element_type=jnp.float32)
    result = (
        result
        + own_weight.astype(jnp.float32)[:, :, None] * value_new.astype(jnp.float32)[:, None, :]
    )
    return result.reshape(-1).astype(jnp.bfloat16)


def expert_ffn(packed_rows, w_gate, w_up, w_down, tensor_sum):
    gate_sum = jnp.dot(packed_rows, w_gate[0], preferred_element_type=jnp.float32)
    up_sum = jnp.dot(packed_rows, w_up[0], preferred_element_type=jnp.float32)
    gate_sum, up_sum = tensor_sum(gate_sum, up_sum)
    activated = (jax.nn.silu(gate_sum) * up_sum).astype(jnp.bfloat16)
    return jnp.dot(activated, w_down[0], preferred_element_type=jnp.float32).astype(jnp.bfloat16)


def add_counts(earlier, later):
    return earlier + later


def shards(
    queries,
    new_keys,
    new_values,
    key_codes,
    key_scale,
    key_zero,
    value_codes,
    value_scale,
    value_zero,
    lengths,
    out_weight,
    residual,
    norm_gain,
    expert_ids,
    route_weights,
    capacity,
    w_gate,
    w_up,
    w_down,
):
    attended = lax.map(
        attend_one,
        (
            queries,
            new_keys,
            new_values,
            key_codes,
            key_scale,
            key_zero,
            value_codes,
            value_scale,
            value_zero,
            lengths,
        ),
    )
    spread = jnp.dot(
        lax.all_gather(attended, ("ep", "sub"), axis=0, tiled=True),
        out_weight,
        preferred_element_type=jnp.float32,
    )
    partial_sum = lax.all_to_all(
        spread.astype(jnp.bfloat16), ("ep", "sub"), split_axis=0, concat_axis=1, tiled=True
    ).astype(spread.dtype)
    quarter = residual.shape[1]
    tp_index = lax.axis_index("tp")
    own_cols = lax.dynamic_slice_in_dim(
        partial_sum, tp_index * quarter, quarter, 1
    ) + residual.astype(jnp.float32)
    placed = lax.dynamic_update_slice_in_dim(partial_sum, own_cols, tp_index * quarter, 1)
    hidden_full = lax.psum(placed.astype(jnp.bfloat16), "tp").astype(jnp.float32)
    hidden_state = lax.dynamic_slice_in_dim(hidden_full, tp_index * quarter, quarter, 1)
    mean_square = jnp.mean(hidden_full * hidden_full, axis=1, keepdims=True)
    normed = (hidden_state * lax.rsqrt(mean_square + EPS) * norm_gain.astype(jnp.float32)).astype(
        jnp.bfloat16
    )
    requests, top_count = expert_ids.shape
    experts_all = capacity.shape[0]
    slot_rows = min(requests, max(2, 5 * requests * top_count // (2 * experts_all)))
    chosen = (expert_ids[:, :, None] == jnp.arange(experts_all, dtype=jnp.int32)).astype(jnp.int32)
    is_named = jnp.sum(chosen, axis=1)
    local_rank = jnp.cumsum(is_named, axis=0) - is_named
    counts = jnp.sum(is_named, axis=0)
    raw_weight = route_weights.astype(jnp.float32)
    shares = raw_weight / jnp.sum(raw_weight, axis=1, keepdims=True)
    weight_per = jnp.sum(chosen.astype(jnp.float32) * shares[:, :, None], axis=1)
    slot_ids = jnp.arange(slot_rows, dtype=jnp.int32)
    at_slot = (local_rank[:, :, None] == slot_ids) & (is_named[:, :, None] > 0)
    offsets = carried_in(counts, ("ep", "sub"), add_counts, jnp.zeros_like(counts))
    kept_rows = offsets[None, :] + local_rank < capacity[None, :]
    send_map = (at_slot & kept_rows[:, :, None]).astype(jnp.bfloat16).reshape(requests, -1)
    outgoing = jnp.dot(send_map.T, normed, preferred_element_type=jnp.float32).astype(jnp.bfloat16)
    outgoing = outgoing.reshape(experts_all, slot_rows, quarter)

    def slot_sums(gate_sum, up_sum):
        return (
            lax.psum(gate_sum.astype(jnp.bfloat16), "tp").astype(jnp.float32),
            lax.psum(up_sum.astype(jnp.bfloat16), "tp").astype(jnp.float32),
        )

    received = lax.all_to_all(outgoing, ("ep", "sub"), split_axis=0, concat_axis=0, tiled=True)
    source_count, item_count, width = received.shape
    expert_out = expert_ffn(received.reshape(-1, width), w_gate, w_up, w_down, slot_sums)
    returned = lax.all_to_all(
        expert_out.reshape(source_count, item_count, width),
        ("ep", "sub"),
        split_axis=0,
        concat_axis=0,
        tiled=True,
    )
    combine_map = (at_slot.astype(jnp.float32) * weight_per[:, :, None]).reshape(requests, -1)
    moe = jnp.dot(
        combine_map,
        returned.reshape(-1, quarter).astype(jnp.float32),
        precision=lax.Precision.HIGHEST,
    )
    return (hidden_state + moe).astype(jnp.bfloat16)


F32, BF16 = jnp.float32, jnp.bfloat16
NT = (((1,), (1,)), ((), ()))
LANES, ROWS = 128, 8


def layer_kernel(
    sizes,
    queries,
    new_keys,
    new_values,
    key_codes,
    key_scale,
    key_zero,
    value_codes,
    value_scale,
    value_zero,
    lengths,
    out_weight_hbm,
    residual,
    norm_gain,
    expert_ids,
    route_weights,
    capacity,
    w_gate_hbm,
    w_up_hbm,
    w_down_hbm,
    mixed,
    out_weight,
    w_gate,
    w_up,
    w_down,
    stage,
    att_send,
    att_recv,
    ids_send,
    ids_recv,
    res_recv,
    proj_send,
    proj_recv,
    hidden,
    norm_send,
    norm_recv,
    sums_own,
    sums_send,
    sums_recv,
    back_send,
    back_recv,
    weight_sem,
    att_ss,
    att_rs,
    ids_ss,
    ids_rs,
    res_ss,
    res_rs,
    proj_ss,
    proj_rs,
    norm_ss,
    norm_rs,
    sums_ss,
    sums_rs,
    back_ss,
    back_rs,
):
    n_tp, n_sub, owners, slots, chunk = sizes
    n_all = owners * n_tp
    tp = lax.axis_index("tp")
    me = lax.axis_index("ep") * n_sub + lax.axis_index("sub")
    requests, heads, head_dim = queries.shape
    kv_heads, words = key_codes.shape[1:3]
    key_groups = key_scale.shape[2]
    per_group = heads // kv_heads
    tokens = owners * requests
    quarter = residual.shape[1]
    tiles = quarter // LANES
    ff = w_gate.shape[1]
    chunks = ff // chunk

    def place(owner, t):
        return {"ep": owner // n_sub, "sub": lax.rem(owner, n_sub), "tp": t}

    def remote(src, dst, ss, rs, owner, t):
        return pltpu.make_async_remote_copy(
            src_ref=src,
            dst_ref=dst,
            send_sem=ss,
            recv_sem=rs,
            device_id=place(owner, t),
            device_id_type=pl.DeviceIdType.MESH,
        )

    def loop(count, body):
        def step(k, carry):
            body(k)
            return carry

        lax.fori_loop(0, count, step, 0)

    barrier = pltpu.get_barrier_semaphore()

    def greet(k):
        other = lax.rem(me * n_tp + tp + k + 1, n_all)
        pl.semaphore_signal(
            barrier,
            inc=1,
            device_id=place(other // n_tp, lax.rem(other, n_tp)),
            device_id_type=pl.DeviceIdType.MESH,
        )

    loop(n_all - 1, greet)
    loads = [
        pltpu.make_async_copy(out_weight_hbm, out_weight, weight_sem.at[0]),
        pltpu.make_async_copy(w_gate_hbm.at[0], w_gate, weight_sem.at[1]),
        pltpu.make_async_copy(w_up_hbm.at[0], w_up, weight_sem.at[2]),
        pltpu.make_async_copy(w_down_hbm.at[0], w_down, weight_sem.at[3]),
    ]
    for load in loads:
        load.start()

    ids = expert_ids[...]
    raw = route_weights[...].astype(F32)
    shares = raw / jnp.sum(raw, axis=1, keepdims=True)
    lane = lax.broadcasted_iota(jnp.int32, (requests, LANES), 1)
    named = jnp.zeros((requests, LANES), F32)
    weight_per = jnp.zeros((requests, LANES), F32)
    for k in range(ids.shape[1]):
        hit = ids[:, k : k + 1] == lane
        named = named + jnp.where(hit, 1.0, 0.0)
        weight_per = weight_per + jnp.where(hit, shares[:, k : k + 1], 0.0)
    ids_send[...] = named
    ids_recv[me] = named
    res_recv[tp] = residual[...]

    def other_owner(k):
        return lax.rem(me + k + 1, owners)

    def other_tp(k):
        return lax.rem(tp + k + 1, n_tp)

    span = words * 16
    row_at = lax.broadcasted_iota(jnp.int32, (span, span), 0)
    col_at = lax.broadcasted_iota(jnp.int32, (span, span), 1)
    moved = 16 * lax.rem(col_at, words) + col_at // words
    perm = jnp.where(row_at == moved, 1.0, 0.0).astype(BF16)
    shifts = 2 * lax.broadcasted_iota(jnp.int32, (16, words, head_dim), 0)
    word_at = lax.broadcasted_iota(jnp.int32, (words, head_dim), 0)
    lane_pos = lax.broadcasted_iota(jnp.int32, (per_group, span), 1)
    position = 16 * lax.rem(lane_pos, words) + lane_pos // words
    inv_scale = 1.0 / math.sqrt(head_dim)

    def per_word(ref, b, g):
        rows = ref[b, g].astype(F32)
        out = rows[0:1, :] * jnp.ones((words, 1), F32)
        for i in range(1, key_groups):
            out = jnp.where(word_at >= i * (words // key_groups), rows[i : i + 1, :], out)
        return out

    v_steps = [
        jnp.dot(value_scale[b], perm, preferred_element_type=F32) for b in range(requests)
    ]
    v_zeros = [jnp.dot(value_zero[b], perm, preferred_element_type=F32) for b in range(requests)]
    for g in range(kv_heads):
        scores, own_scores = [], []
        for b in range(requests):
            code = jnp.bitwise_and(jnp.right_shift(key_codes[b, g][None], shifts), 3).astype(F32)
            keys = code * per_word(key_scale, b, g)[None] + per_word(key_zero, b, g)[None]
            keys = keys.reshape(span, head_dim).astype(BF16)
            q = queries[b, g * per_group : (g + 1) * per_group, :]
            s = lax.dot_general(q, keys, NT, preferred_element_type=F32) * inv_scale
            scores.append(jnp.where(position < lengths[b], s, -jnp.inf))
            nk = new_keys[b, g : g + 1, :].astype(F32)
            own_scores.append(jnp.sum(q.astype(F32) * nk, axis=1, keepdims=True) * inv_scale)
        score = jnp.concatenate(scores, axis=0)
        own = jnp.concatenate(own_scores, axis=0)
        highest = jnp.maximum(jnp.max(score, axis=1, keepdims=True), own)
        weights = jnp.exp(score - highest)
        own_w = jnp.exp(own - highest)
        inverse = 1.0 / (jnp.sum(weights, axis=1, keepdims=True) + own_w)
        weights = weights * inverse
        own_w = own_w * inverse
        for b in range(requests):
            p = weights[b * per_group : (b + 1) * per_group, :]
            o = own_w[b * per_group : (b + 1) * per_group, :]
            code = jnp.bitwise_and(jnp.right_shift(value_codes[b, g][None], shifts), 3)
            code = code.astype(F32).reshape(span, head_dim).astype(BF16)
            ps = (p * v_steps[b][g : g + 1, :]).astype(BF16)
            res = jnp.dot(ps, code, preferred_element_type=F32)
            res = res + jnp.sum(p * v_zeros[b][g : g + 1, :], axis=1, keepdims=True)
            res = res + o * new_values[b, g : g + 1, :].astype(F32)
            stage[g, pl.ds(b, per_group, stride=requests), :] = res
        done = stage[g].astype(BF16)
        att_send[g] = done
        att_recv[me, g] = done
        if g == 0:
            pl.semaphore_wait(barrier, n_all - 1)

        def send_att(k):
            p = other_owner(k)
            remote(
                att_send.at[g], att_recv.at[me, g], att_ss.at[g, k], att_rs.at[g, me], p, tp
            ).start()

        loop(owners - 1, send_att)

    def send_ids(k):
        remote(ids_send, ids_recv.at[me], ids_ss.at[k], ids_rs.at[me], other_owner(k), tp).start()

    def send_res(k):
        remote(residual, res_recv.at[tp], res_ss.at[k], res_rs.at[tp], me, other_tp(k)).start()

    loop(n_tp - 1, send_res)
    loop(owners - 1, send_ids)

    loads[0].wait()
    spread = jnp.zeros((tokens, LANES), F32)
    for g in range(kv_heads):

        def got_att(k):
            s = other_owner(k)
            remote(
                att_send.at[g], att_recv.at[s, g], att_ss.at[g, k], att_rs.at[g, s], s, tp
            ).wait_recv()

        loop(owners - 1, got_att)
        got = att_recv[:, g].astype(F32).reshape(owners, per_group, requests, head_dim)
        lhs = [got[:, h].reshape(tokens, head_dim).astype(BF16) for h in range(per_group)]
        width = per_group * head_dim
        spread = spread + jnp.dot(
            jnp.concatenate(lhs, axis=1),
            out_weight[g * width : (g + 1) * width, :],
            preferred_element_type=F32,
        )
    proj_send[...] = spread.reshape(owners, requests, LANES).astype(BF16)
    proj_recv[tp, me] = proj_send[me]

    def pair(k):
        other = lax.rem(me * n_tp + tp + k + 1, n_all)
        return other // n_tp, lax.rem(other, n_tp)

    def send_proj(k):
        p, t = pair(k)
        remote(
            proj_send.at[p], proj_recv.at[tp, me], proj_ss.at[k], proj_rs.at[tp, me], p, t
        ).start()

    loop(n_all - 1, send_proj)

    def got_ids(k):
        s = other_owner(k)
        remote(ids_send, ids_recv.at[s], ids_ss.at[k], ids_rs.at[s], s, tp).wait_recv()

    loop(owners - 1, got_ids)
    named_all = ids_recv[...].reshape(tokens, LANES)
    before = lax.broadcasted_iota(jnp.int32, (tokens, tokens), 0) > lax.broadcasted_iota(
        jnp.int32, (tokens, tokens), 1
    )
    rank = jnp.dot(
        jnp.where(before, 1.0, 0.0).astype(BF16),
        named_all.astype(BF16),
        preferred_element_type=F32,
    )
    limit = capacity[me].astype(F32)
    ranked = jnp.where((named_all > 0.5) & (rank < limit), rank, -1.0)
    mine = lax.broadcasted_iota(jnp.int32, (tokens, LANES), 1) == me
    rank_col = jnp.sum(jnp.where(mine, ranked, 0.0), axis=1, keepdims=True)
    pick = jnp.where(lax.broadcasted_iota(jnp.int32, (ROWS, LANES), 1) == me, 1.0, 0.0)
    rank_row = lax.dot_general(
        pick.astype(BF16), ranked.astype(BF16), NT, preferred_element_type=F32
    )[0:1, :]
    slot_row = lax.broadcasted_iota(jnp.int32, (slots, tokens), 0).astype(F32)
    slot_col = lax.broadcasted_iota(jnp.int32, (tokens, slots), 1).astype(F32)
    packer = jnp.where(rank_row == slot_row, 1.0, 0.0).astype(BF16)
    unpacker = jnp.where(rank_col == slot_col, 1.0, 0.0).astype(BF16)

    def got_res(k):
        t = other_tp(k)
        remote(residual, res_recv.at[t], res_ss.at[k], res_rs.at[t], me, t).wait_recv()

    loop(n_tp - 1, got_res)

    def got_proj(k):
        s, t = pair(k)
        remote(
            proj_send.at[s], proj_recv.at[t, s], proj_ss.at[k], proj_rs.at[t, s], s, t
        ).wait_recv()

    loop(n_all - 1, got_proj)
    total = proj_recv[0].astype(F32)
    for t in range(1, n_tp):
        total = total + proj_recv[t].astype(F32)
    squares = jnp.zeros((requests, LANES), F32)
    for i in range(owners):
        t, k = divmod(i, tiles)
        h = total[i] + res_recv[t, :, k * LANES : (k + 1) * LANES].astype(F32)
        hidden[t, k] = h
        squares = squares + h * h
    mean_square = jnp.sum(squares, axis=1, keepdims=True) * (1.0 / (owners * LANES))
    inv_rms = lax.rsqrt(mean_square + EPS)
    own_hidden = hidden[tp]
    normed = [
        own_hidden[k] * inv_rms * norm_gain[:, k * LANES : (k + 1) * LANES].astype(F32)
        for k in range(tiles)
    ]
    normed = jnp.concatenate(normed, axis=0).astype(BF16)
    norm_send[...] = normed
    norm_recv[me] = normed

    def send_norm(k):
        remote(
            norm_send, norm_recv.at[me], norm_ss.at[k], norm_rs.at[me], other_owner(k), tp
        ).start()

    loop(owners - 1, send_norm)
    loads[1].wait()
    loads[2].wait()
    loads[3].wait()

    def got_norm(k):
        s = other_owner(k)
        remote(norm_send, norm_recv.at[s], norm_ss.at[k], norm_rs.at[s], s, tp).wait_recv()

    loop(owners - 1, got_norm)
    got = norm_recv[...].astype(F32).reshape(owners, tiles, requests, LANES)
    rows = [got[:, k].reshape(tokens, LANES).astype(BF16) for k in range(tiles)]
    packed = jnp.dot(
        packer, jnp.concatenate(rows, axis=1), preferred_element_type=F32
    ).astype(BF16)
    for c in range(chunks):
        cols = slice(c * chunk, (c + 1) * chunk)
        both = jnp.concatenate(
            [
                jnp.dot(packed, w_gate[:, cols], preferred_element_type=F32),
                jnp.dot(packed, w_up[:, cols], preferred_element_type=F32),
            ],
            axis=1,
        )
        sums_own[c] = both
        sums_send[c] = both.astype(BF16)

        def send_sums(k):
            remote(
                sums_send.at[c],
                sums_recv.at[tp, c],
                sums_ss.at[c, k],
                sums_rs.at[c, tp],
                me,
                other_tp(k),
            ).start()

        loop(n_tp - 1, send_sums)
    expert_out = jnp.zeros((slots, quarter), F32)
    for c in range(chunks):
        both = sums_own[c]
        for k in range(n_tp - 1):
            t = other_tp(k)
            remote(
                sums_send.at[c], sums_recv.at[t, c], sums_ss.at[c, k], sums_rs.at[c, t], me, t
            ).wait_recv()
            both = both + sums_recv[t, c].astype(F32)
        gate, up = both[:, :chunk], both[:, chunk:]
        activated = (gate / (1.0 + jnp.exp(-gate)) * up).astype(BF16)
        expert_out = expert_out + jnp.dot(
            activated, w_down[c * chunk : (c + 1) * chunk, :], preferred_element_type=F32
        )
    spread_back = jnp.dot(unpacker, expert_out.astype(BF16), preferred_element_type=F32)
    for r in range(owners):
        part = [
            spread_back[r * requests : (r + 1) * requests, k * LANES : (k + 1) * LANES]
            for k in range(tiles)
        ]
        back_send[r] = jnp.concatenate(part, axis=0).astype(BF16)
    back_recv[me] = back_send[me]

    def send_back(k):
        p = other_owner(k)
        remote(
            back_send.at[p], back_recv.at[me], back_ss.at[k], back_rs.at[me], p, tp
        ).start()

    loop(owners - 1, send_back)

    def got_back(k):
        s = other_owner(k)
        remote(back_send.at[s], back_recv.at[s], back_ss.at[k], back_rs.at[s], s, tp).wait_recv()

    loop(owners - 1, got_back)
    moe = own_hidden
    for e in range(owners):
        part = back_recv[e].astype(F32).reshape(tiles, requests, LANES)
        moe = moe + part * weight_per[:, e : e + 1][None]
    for k in range(tiles):
        mixed[:, k * LANES : (k + 1) * LANES] = moe[k].astype(BF16)

    def sent_owner(k):
        p = other_owner(k)
        for g in range(kv_heads):
            remote(
                att_send.at[g], att_recv.at[me, g], att_ss.at[g, k], att_rs.at[g, me], p, tp
            ).wait_send()
        remote(ids_send, ids_recv.at[me], ids_ss.at[k], ids_rs.at[me], p, tp).wait_send()
        remote(norm_send, norm_recv.at[me], norm_ss.at[k], norm_rs.at[me], p, tp).wait_send()
        remote(
            back_send.at[p], back_recv.at[me], back_ss.at[k], back_rs.at[me], p, tp
        ).wait_send()

    def sent_tp(k):
        t = other_tp(k)
        remote(residual, res_recv.at[tp], res_ss.at[k], res_rs.at[tp], me, t).wait_send()
        for c in range(chunks):
            remote(
                sums_send.at[c], sums_recv.at[tp, c], sums_ss.at[c, k], sums_rs.at[c, tp], me, t
            ).wait_send()

    def sent_proj(k):
        p, t = pair(k)
        remote(
            proj_send.at[p], proj_recv.at[tp, me], proj_ss.at[k], proj_rs.at[tp, me], p, t
        ).wait_send()

    loop(owners - 1, sent_owner)
    loop(n_tp - 1, sent_tp)
    loop(n_all - 1, sent_proj)


def fused_shards(n_ep, n_tp, n_sub, *args):
    owners = n_ep * n_sub
    queries, key_codes, out_weight, residual = args[0], args[3], args[10], args[11]
    norm_gain, expert_ids, capacity, w_gate, w_down = (
        args[12],
        args[13],
        args[15],
        args[16],
        args[18],
    )
    requests, heads, head_dim = queries.shape
    kv_heads = key_codes.shape[1]
    quarter, ff = residual.shape[1], w_gate.shape[2]
    tiles = quarter // LANES
    tokens = owners * requests
    slots = tokens * expert_ids.shape[1] // (2 * owners)
    chunk = 256
    chunks = ff // chunk
    group_rows = heads // kv_heads * requests
    vmem, dma = pltpu.VMEM, pltpu.SemaphoreType.DMA
    in_vmem = pl.BlockSpec(memory_space=pltpu.VMEM)
    in_smem = pl.BlockSpec(memory_space=pltpu.SMEM)
    in_any = pl.BlockSpec(memory_space=pl.ANY)
    specs = [in_vmem] * 9 + [in_smem, in_any] + [in_vmem] * 4 + [in_smem] + [in_any] * 3
    args = list(args)
    args[12] = norm_gain.reshape(1, -1)
    return pl.pallas_call(
        functools.partial(layer_kernel, (n_tp, n_sub, owners, slots, chunk)),
        out_shape=jax.ShapeDtypeStruct(residual.shape, BF16),
        in_specs=specs,
        out_specs=in_vmem,
        scratch_shapes=[
            vmem(out_weight.shape, BF16),
            vmem(w_gate.shape[1:], BF16),
            vmem(w_gate.shape[1:], BF16),
            vmem(w_down.shape[1:], BF16),
            vmem((kv_heads, group_rows, head_dim), F32),
            vmem((kv_heads, group_rows, head_dim), BF16),
            vmem((owners, kv_heads, group_rows, head_dim), BF16),
            vmem((requests, LANES), F32),
            vmem((owners, requests, LANES), F32),
            vmem((n_tp, requests, quarter), BF16),
            vmem((owners, requests, LANES), BF16),
            vmem((n_tp, owners, requests, LANES), BF16),
            vmem((n_tp, tiles, requests, LANES), F32),
            vmem((tiles * requests, LANES), BF16),
            vmem((owners, tiles * requests, LANES), BF16),
            vmem((chunks, slots, 2 * chunk), F32),
            vmem((chunks, slots, 2 * chunk), BF16),
            vmem((n_tp, chunks, slots, 2 * chunk), BF16),
            vmem((owners, tiles * requests, LANES), BF16),
            vmem((owners, tiles * requests, LANES), BF16),
            dma((4,)),
            dma((kv_heads, owners)),
            dma((kv_heads, owners)),
            dma((owners,)),
            dma((owners,)),
            dma((n_tp,)),
            dma((n_tp,)),
            dma((owners * n_tp,)),
            dma((n_tp, owners)),
            dma((owners,)),
            dma((owners,)),
            dma((chunks, n_tp)),
            dma((chunks, n_tp)),
            dma((owners,)),
            dma((owners,)),
        ],
        compiler_params=pltpu.CompilerParams(collective_id=0, has_side_effects=True),
    )(*args)


def layer(n_ep, n_tp, n_sub, *args):
    requests, heads, head_dim = args[0].shape
    fits = (
        requests == ROWS
        and head_dim == LANES
        and args[3].shape[2] * 16 == LANES
        and (heads // args[3].shape[1]) % 16 == 0
        and args[10].shape[1] == LANES
        and args[11].shape[1] * n_tp == n_ep * n_sub * LANES
        and args[16].shape[0] == 1
        and n_ep * n_sub == args[15].shape[0]
        and n_ep * n_sub * requests == LANES
    )
    return fused_shards(n_ep, n_tp, n_sub, *args) if fits else shards(*args)


def solution(mesh):
    sizes = [mesh.shape[axis] for axis in ("ep", "tp", "sub")]
    return jax.shard_map(
        functools.partial(layer, *sizes),
        mesh=mesh,
        in_specs=(
            P(("groups", "ep", "sub"), "tp", None),
            P(("groups", "ep", "sub"), "tp", None),
            P(("groups", "ep", "sub"), "tp", None),
            P(("groups", "ep", "sub"), "tp", None, None),
            P(("groups", "ep", "sub"), "tp", None, None),
            P(("groups", "ep", "sub"), "tp", None, None),
            P(("groups", "ep", "sub"), "tp", None, None),
            P(("groups", "ep", "sub"), "tp", None),
            P(("groups", "ep", "sub"), "tp", None),
            P(("groups", "ep", "sub")),
            P("tp", ("ep", "sub")),
            P(("groups", "ep", "sub"), "tp"),
            P("tp"),
            P(("groups", "ep", "sub"), None),
            P(("groups", "ep", "sub"), None),
            P("groups"),
            P(("ep", "sub"), "tp", None),
            P(("ep", "sub"), "tp", None),
            P(("ep", "sub"), None, "tp"),
        ),
        out_specs=P(("groups", "ep", "sub"), "tp"),
        check_vma=False,
    )
```

```python
import functools
import math

import jax
import jax.numpy as jnp
from jax import lax
from jax.experimental import pallas as pl
from jax.experimental.pallas import tpu as pltpu
from jax.sharding import PartitionSpec as P

EPS = 1e-06


def carried_in(value, axis, join, neutral):
    count, mine = (lax.axis_size(axis), lax.axis_index(axis))
    pieces = lax.all_gather(value, axis)
    total = jnp.full_like(value, 0) + jnp.asarray(neutral, value.dtype)

    def turn(position, total):
        longer = join(total, pieces[position])
        return jnp.where(position < mine, longer, total)

    return lax.fori_loop(0, count - 1, turn, total)


def unpack_codes(packed_words):
    shifts = 2 * jnp.arange(16)
    code_vals = jnp.bitwise_and(jnp.right_shift(packed_words[..., None, :], shifts[:, None]), 3)
    word_shape = packed_words.shape
    return code_vals.reshape(word_shape[:-2] + (word_shape[-2] * 16, word_shape[-1])).astype(
        jnp.float32
    )


def attend_one(request_data):
    (
        query_heads,
        key_new,
        value_new,
        key_words,
        key_step,
        key_offset,
        value_words,
        value_step,
        value_offset,
        seq_length,
    ) = request_data
    kv_heads, head_dim = key_new.shape
    token_group = key_words.shape[1] * 16 // key_step.shape[1]
    keys_deq = unpack_codes(key_words) * jnp.repeat(
        key_step.astype(jnp.float32), token_group, axis=1
    )
    keys_deq = (keys_deq + jnp.repeat(key_offset.astype(jnp.float32), token_group, axis=1)).astype(
        jnp.bfloat16
    )
    values_deq = (
        unpack_codes(value_words) * value_step.astype(jnp.float32)[:, :, None]
        + value_offset.astype(jnp.float32)[:, :, None]
    )
    values_deq = values_deq.astype(jnp.bfloat16)
    grouped = query_heads.reshape(kv_heads, -1, head_dim)
    inv_scale = 1.0 / math.sqrt(head_dim)
    scores = (
        jnp.einsum("kgd,kld->kgl", grouped, keys_deq, preferred_element_type=jnp.float32)
        * inv_scale
    )
    own_score = (
        jnp.einsum("kgd,kd->kg", grouped, key_new, preferred_element_type=jnp.float32) * inv_scale
    )
    usable = jnp.arange(keys_deq.shape[1]) < seq_length
    scores = jnp.where(usable, scores, -jnp.inf)
    highest = jnp.maximum(jnp.max(scores, axis=2), own_score)
    weights = jnp.exp(scores - highest[:, :, None])
    own_weight = jnp.exp(own_score - highest)
    totals = jnp.sum(weights, axis=2) + own_weight
    weights = (weights / totals[:, :, None]).astype(jnp.bfloat16)
    own_weight = (own_weight / totals).astype(jnp.bfloat16)
    result = jnp.einsum("kgl,kld->kgd", weights, values_deq, preferred_element_type=jnp.float32)
    result = (
        result
        + own_weight.astype(jnp.float32)[:, :, None] * value_new.astype(jnp.float32)[:, None, :]
    )
    return result.reshape(-1).astype(jnp.bfloat16)


def expert_ffn(packed_rows, w_gate, w_up, w_down, tensor_sum):
    gate_sum = jnp.dot(packed_rows, w_gate[0], preferred_element_type=jnp.float32)
    up_sum = jnp.dot(packed_rows, w_up[0], preferred_element_type=jnp.float32)
    gate_sum, up_sum = tensor_sum(gate_sum, up_sum)
    activated = (jax.nn.silu(gate_sum) * up_sum).astype(jnp.bfloat16)
    return jnp.dot(activated, w_down[0], preferred_element_type=jnp.float32).astype(jnp.bfloat16)


def add_counts(earlier, later):
    return earlier + later


def shards(
    queries,
    new_keys,
    new_values,
    key_codes,
    key_scale,
    key_zero,
    value_codes,
    value_scale,
    value_zero,
    lengths,
    out_weight,
    residual,
    norm_gain,
    expert_ids,
    route_weights,
    capacity,
    w_gate,
    w_up,
    w_down,
):
    attended = lax.map(
        attend_one,
        (
            queries,
            new_keys,
            new_values,
            key_codes,
            key_scale,
            key_zero,
            value_codes,
            value_scale,
            value_zero,
            lengths,
        ),
    )
    spread = jnp.dot(
        lax.all_gather(attended, ("ep", "sub"), axis=0, tiled=True),
        out_weight,
        preferred_element_type=jnp.float32,
    )
    partial_sum = lax.all_to_all(
        spread.astype(jnp.bfloat16), ("ep", "sub"), split_axis=0, concat_axis=1, tiled=True
    ).astype(spread.dtype)
    quarter = residual.shape[1]
    tp_index = lax.axis_index("tp")
    own_cols = lax.dynamic_slice_in_dim(
        partial_sum, tp_index * quarter, quarter, 1
    ) + residual.astype(jnp.float32)
    placed = lax.dynamic_update_slice_in_dim(partial_sum, own_cols, tp_index * quarter, 1)
    hidden_full = lax.psum(placed.astype(jnp.bfloat16), "tp").astype(jnp.float32)
    hidden_state = lax.dynamic_slice_in_dim(hidden_full, tp_index * quarter, quarter, 1)
    mean_square = jnp.mean(hidden_full * hidden_full, axis=1, keepdims=True)
    normed = (hidden_state * lax.rsqrt(mean_square + EPS) * norm_gain.astype(jnp.float32)).astype(
        jnp.bfloat16
    )
    requests, top_count = expert_ids.shape
    experts_all = capacity.shape[0]
    slot_rows = min(requests, max(2, 5 * requests * top_count // (2 * experts_all)))
    chosen = (expert_ids[:, :, None] == jnp.arange(experts_all, dtype=jnp.int32)).astype(jnp.int32)
    is_named = jnp.sum(chosen, axis=1)
    local_rank = jnp.cumsum(is_named, axis=0) - is_named
    counts = jnp.sum(is_named, axis=0)
    raw_weight = route_weights.astype(jnp.float32)
    shares = raw_weight / jnp.sum(raw_weight, axis=1, keepdims=True)
    weight_per = jnp.sum(chosen.astype(jnp.float32) * shares[:, :, None], axis=1)
    slot_ids = jnp.arange(slot_rows, dtype=jnp.int32)
    at_slot = (local_rank[:, :, None] == slot_ids) & (is_named[:, :, None] > 0)
    offsets = carried_in(counts, ("ep", "sub"), add_counts, jnp.zeros_like(counts))
    kept_rows = offsets[None, :] + local_rank < capacity[None, :]
    send_map = (at_slot & kept_rows[:, :, None]).astype(jnp.bfloat16).reshape(requests, -1)
    outgoing = jnp.dot(send_map.T, normed, preferred_element_type=jnp.float32).astype(jnp.bfloat16)
    outgoing = outgoing.reshape(experts_all, slot_rows, quarter)

    def slot_sums(gate_sum, up_sum):
        return (
            lax.psum(gate_sum.astype(jnp.bfloat16), "tp").astype(jnp.float32),
            lax.psum(up_sum.astype(jnp.bfloat16), "tp").astype(jnp.float32),
        )

    received = lax.all_to_all(outgoing, ("ep", "sub"), split_axis=0, concat_axis=0, tiled=True)
    source_count, item_count, width = received.shape
    expert_out = expert_ffn(received.reshape(-1, width), w_gate, w_up, w_down, slot_sums)
    returned = lax.all_to_all(
        expert_out.reshape(source_count, item_count, width),
        ("ep", "sub"),
        split_axis=0,
        concat_axis=0,
        tiled=True,
    )
    combine_map = (at_slot.astype(jnp.float32) * weight_per[:, :, None]).reshape(requests, -1)
    moe = jnp.dot(
        combine_map,
        returned.reshape(-1, quarter).astype(jnp.float32),
        precision=lax.Precision.HIGHEST,
    )
    return (hidden_state + moe).astype(jnp.bfloat16)


F32, BF16 = jnp.float32, jnp.bfloat16
NT = (((1,), (1,)), ((), ()))
LANES, ROWS = 128, 8


def layer_kernel(
    sizes,
    queries,
    new_keys,
    new_values,
    key_codes,
    key_scale,
    key_zero,
    value_codes,
    value_scale,
    value_zero,
    lengths,
    out_weight_hbm,
    residual,
    norm_gain,
    expert_ids,
    route_weights,
    capacity,
    w_gate_hbm,
    w_up_hbm,
    w_down_hbm,
    mixed,
    out_weight,
    w_gate,
    w_up,
    w_down,
    stage,
    att_recv,
    ids_send,
    ids_recv,
    res_recv,
    proj_send,
    proj_recv,
    hidden,
    norm_recv,
    sums_own,
    sums_send,
    sums_recv,
    back_send,
    back_recv,
    weight_sem,
    att_ss,
    att_rs,
    ids_ss,
    ids_rs,
    res_ss,
    res_rs,
    proj_ss,
    proj_rs,
    norm_ss,
    norm_rs,
    sums_ss,
    sums_rs,
    back_ss,
    back_rs,
):
    n_tp, n_sub, owners, slots, chunk = sizes
    n_all = owners * n_tp
    tp = lax.axis_index("tp")
    me = lax.axis_index("ep") * n_sub + lax.axis_index("sub")
    requests, heads, head_dim = queries.shape
    kv_heads, words = key_codes.shape[1:3]
    key_groups = key_scale.shape[2]
    per_group = heads // kv_heads
    tokens = owners * requests
    quarter = residual.shape[1]
    tiles = quarter // LANES
    ff = w_gate.shape[1]
    chunks = ff // chunk

    def place(owner, t):
        return {"ep": owner // n_sub, "sub": lax.rem(owner, n_sub), "tp": t}

    def remote(src, dst, ss, rs, owner, t):
        return pltpu.make_async_remote_copy(
            src_ref=src,
            dst_ref=dst,
            send_sem=ss,
            recv_sem=rs,
            device_id=place(owner, t),
            device_id_type=pl.DeviceIdType.MESH,
        )

    def loop(count, body):
        def step(k, carry):
            body(k)
            return carry

        lax.fori_loop(0, count, step, 0)

    barrier = pltpu.get_barrier_semaphore()

    def greet(k):
        other = lax.rem(me * n_tp + tp + k + 1, n_all)
        pl.semaphore_signal(
            barrier,
            inc=1,
            device_id=place(other // n_tp, lax.rem(other, n_tp)),
            device_id_type=pl.DeviceIdType.MESH,
        )

    loop(n_all - 1, greet)
    loads = [
        pltpu.make_async_copy(out_weight_hbm, out_weight, weight_sem.at[0]),
        pltpu.make_async_copy(w_gate_hbm.at[0], w_gate, weight_sem.at[1]),
        pltpu.make_async_copy(w_up_hbm.at[0], w_up, weight_sem.at[2]),
        pltpu.make_async_copy(w_down_hbm.at[0], w_down, weight_sem.at[3]),
    ]
    for load in loads:
        load.start()

    ids = expert_ids[...]
    raw = route_weights[...].astype(F32)
    shares = raw / jnp.sum(raw, axis=1, keepdims=True)
    lane = lax.broadcasted_iota(jnp.int32, (requests, LANES), 1)
    named = jnp.zeros((requests, LANES), F32)
    weight_per = jnp.zeros((requests, LANES), F32)
    for k in range(ids.shape[1]):
        hit = ids[:, k : k + 1] == lane
        named = named + jnp.where(hit, 1.0, 0.0)
        weight_per = weight_per + jnp.where(hit, shares[:, k : k + 1], 0.0)
    ids_send[...] = named
    ids_recv[me] = named
    res_recv[tp] = residual[...]

    def other_owner(k):
        return lax.rem(me + k + 1, owners)

    def other_tp(k):
        return lax.rem(tp + k + 1, n_tp)

    drains = []

    def finish():
        for item in drains:
            if isinstance(item, tuple):
                loop(*item)
            else:
                item.wait_send()
        for load in left:
            load.wait()

    left = list(loads)

    near = 2 if (owners // n_sub) % 2 == 0 else 1
    row = near * n_sub
    far = owners // row
    my_far, my_near, my_sub = me // row, lax.rem(me // n_sub, near), lax.rem(me, n_sub)

    def owner_at(f, y, u):
        return (
            lax.rem(my_far + f, far) * row
            + lax.rem(my_near + y, near) * n_sub
            + lax.rem(my_sub + u, n_sub)
        )

    def hand_on(part, block, slot, target):
        view, ss, rs = part
        copy = remote(view(block), view(block), ss(slot), rs(block), target, tp)
        copy.start()
        drains.append(copy)

    def arrived(part, block):
        view, ss, rs = part
        remote(view(block), view(block), ss(0), rs(block), block, tp).wait_recv()

    def start_gather(part):
        for u in range(1, n_sub):
            hand_on(part, me, far - 1 + u - 1, owner_at(0, 0, u))
        for f in range(1, far):
            hand_on(part, me, f - 1, owner_at(f, 0, 0))
        for y in range(1, near):
            hand_on(part, me, far - 1 + n_sub - 1 + y - 1, owner_at(0, y, 0))

    def finish_gather(parts):
        slot = far - 1 + n_sub - 1 + near - 1
        for f in range(1, far):
            for part in parts:
                block = owner_at(f, 0, 0)
                arrived(part, block)
                for y in range(1, near):
                    hand_on(part, block, slot + (f - 1) * (near - 1) + y - 1, owner_at(0, y, 0))
        slot = slot + (far - 1) * (near - 1)
        for f in range(0, far):
            for y in range(0, near):
                if f == 0 and y == 0:
                    continue
                for part in parts:
                    block = owner_at(f, y, 0)
                    if y > 0:
                        arrived(part, block)
                    for u in range(1, n_sub):
                        hand_on(
                            part,
                            block,
                            slot + (f * near + y - 1) * (n_sub - 1) + u - 1,
                            owner_at(0, 0, u),
                        )
        for f in range(0, far):
            for y in range(0, near):
                for u in range(1, n_sub):
                    for part in parts:
                        arrived(part, owner_at(f, y, u))

    def start_near(part):
        for u in range(1, n_sub):
            hand_on(part, me, u - 1, owner_at(0, 0, u))
        for j in range(1, far * near):
            hand_on(part, me, n_sub - 1 + j - 1, owner_at(j // near, j % near, 0))

    def finish_near(part):
        slot = n_sub - 1 + far * near - 1
        for j in range(1, far * near):
            block = owner_at(j // near, j % near, 0)
            arrived(part, block)
            for u in range(1, n_sub):
                hand_on(part, block, slot + (j - 1) * (n_sub - 1) + u - 1, owner_at(0, 0, u))
        for j in range(far * near):
            for u in range(1, n_sub):
                arrived(part, owner_at(j // near, j % near, u))

    def att_part(g):
        return (
            lambda block: att_recv.at[block, g],
            lambda slot: att_ss.at[g, slot],
            lambda block: att_rs.at[g, block],
        )

    norm_part = (
        lambda block: norm_recv.at[block],
        lambda slot: norm_ss.at[slot],
        lambda block: norm_rs.at[block],
    )

    span = words * 16
    row_at = lax.broadcasted_iota(jnp.int32, (span, span), 0)
    col_at = lax.broadcasted_iota(jnp.int32, (span, span), 1)
    moved = 16 * lax.rem(col_at, words) + col_at // words
    perm = jnp.where(row_at == moved, 1.0, 0.0).astype(BF16)
    shifts = 2 * lax.broadcasted_iota(jnp.int32, (16, words, head_dim), 0)
    word_at = lax.broadcasted_iota(jnp.int32, (words, head_dim), 0)
    lane_pos = lax.broadcasted_iota(jnp.int32, (per_group, span), 1)
    position = 16 * lax.rem(lane_pos, words) + lane_pos // words
    inv_scale = 1.0 / math.sqrt(head_dim)

    def per_word(ref, b, g):
        rows = ref[b, g].astype(F32)
        out = rows[0:1, :] * jnp.ones((words, 1), F32)
        for i in range(1, key_groups):
            out = jnp.where(word_at >= i * (words // key_groups), rows[i : i + 1, :], out)
        return out

    v_steps = [
        jnp.dot(value_scale[b], perm, preferred_element_type=F32) for b in range(requests)
    ]
    v_zeros = [jnp.dot(value_zero[b], perm, preferred_element_type=F32) for b in range(requests)]
    for g in range(kv_heads):
        scores, own_scores = [], []
        for b in range(requests):
            code = jnp.bitwise_and(jnp.right_shift(key_codes[b, g][None], shifts), 3).astype(F32)
            keys = code * per_word(key_scale, b, g)[None] + per_word(key_zero, b, g)[None]
            keys = keys.reshape(span, head_dim).astype(BF16)
            q = queries[b, g * per_group : (g + 1) * per_group, :]
            s = lax.dot_general(q, keys, NT, preferred_element_type=F32) * inv_scale
            scores.append(jnp.where(position < lengths[b], s, -jnp.inf))
            nk = new_keys[b, g : g + 1, :].astype(F32)
            own_scores.append(jnp.sum(q.astype(F32) * nk, axis=1, keepdims=True) * inv_scale)
        score = jnp.concatenate(scores, axis=0)
        own = jnp.concatenate(own_scores, axis=0)
        highest = jnp.maximum(jnp.max(score, axis=1, keepdims=True), own)
        weights = jnp.exp(score - highest)
        own_w = jnp.exp(own - highest)
        inverse = 1.0 / (jnp.sum(weights, axis=1, keepdims=True) + own_w)
        weights = weights * inverse
        own_w = own_w * inverse
        for b in range(requests):
            p = weights[b * per_group : (b + 1) * per_group, :]
            o = own_w[b * per_group : (b + 1) * per_group, :]
            code = jnp.bitwise_and(jnp.right_shift(value_codes[b, g][None], shifts), 3)
            code = code.astype(F32).reshape(span, head_dim).astype(BF16)
            ps = (p * v_steps[b][g : g + 1, :]).astype(BF16)
            res = jnp.dot(ps, code, preferred_element_type=F32)
            res = res + jnp.sum(p * v_zeros[b][g : g + 1, :], axis=1, keepdims=True)
            res = res + o * new_values[b, g : g + 1, :].astype(F32)
            stage[g, pl.ds(b, per_group, stride=requests), :] = res
        att_recv[me, g] = stage[g].astype(BF16)
        if g == 0:
            pl.semaphore_wait(barrier, n_all - 1)

        start_gather(att_part(g))

    def send_ids(k):
        remote(ids_send, ids_recv.at[me], ids_ss.at[k], ids_rs.at[me], other_owner(k), tp).start()

    def send_res(k):
        remote(residual, res_recv.at[tp], res_ss.at[k], res_rs.at[tp], me, other_tp(k)).start()

    loop(n_tp - 1, send_res)
    loop(owners - 1, send_ids)

    def sent_res(k):
        t = other_tp(k)
        remote(residual, res_recv.at[tp], res_ss.at[k], res_rs.at[tp], me, t).wait_send()

    def sent_ids(k):
        p = other_owner(k)
        remote(ids_send, ids_recv.at[me], ids_ss.at[k], ids_rs.at[me], p, tp).wait_send()

    drains += [(n_tp - 1, sent_res), (owners - 1, sent_ids)]

    left.pop(0).wait()
    spread = jnp.zeros((tokens, LANES), F32)
    finish_gather([att_part(g) for g in range(kv_heads)])
    for g in range(kv_heads):
        got = att_recv[:, g].astype(F32).reshape(owners, per_group, requests, head_dim)
        lhs = [got[:, h].reshape(tokens, head_dim).astype(BF16) for h in range(per_group)]
        width = per_group * head_dim
        spread = spread + jnp.dot(
            jnp.concatenate(lhs, axis=1),
            out_weight[g * width : (g + 1) * width, :],
            preferred_element_type=F32,
        )
    proj_send[...] = spread.reshape(owners, requests, LANES).astype(BF16)
    proj_recv[tp, me] = proj_send[me]

    def pair(k):
        other = lax.rem(me * n_tp + tp + k + 1, n_all)
        return other // n_tp, lax.rem(other, n_tp)

    def send_proj(k):
        p, t = pair(k)
        remote(
            proj_send.at[p], proj_recv.at[tp, me], proj_ss.at[k], proj_rs.at[tp, me], p, t
        ).start()

    loop(n_all - 1, send_proj)

    def sent_proj(k):
        p, t = pair(k)
        remote(
            proj_send.at[p], proj_recv.at[tp, me], proj_ss.at[k], proj_rs.at[tp, me], p, t
        ).wait_send()

    drains.append((n_all - 1, sent_proj))

    def got_ids(k):
        s = other_owner(k)
        remote(ids_send, ids_recv.at[s], ids_ss.at[k], ids_rs.at[s], s, tp).wait_recv()

    loop(owners - 1, got_ids)
    named_all = ids_recv[...].reshape(tokens, LANES)
    before = lax.broadcasted_iota(jnp.int32, (tokens, tokens), 0) > lax.broadcasted_iota(
        jnp.int32, (tokens, tokens), 1
    )
    rank = jnp.dot(
        jnp.where(before, 1.0, 0.0).astype(BF16),
        named_all.astype(BF16),
        preferred_element_type=F32,
    )
    limit = capacity[me].astype(F32)
    ranked = jnp.where((named_all > 0.5) & (rank < limit), rank, -1.0)
    mine = lax.broadcasted_iota(jnp.int32, (tokens, LANES), 1) == me
    rank_col = jnp.sum(jnp.where(mine, ranked, 0.0), axis=1, keepdims=True)
    pick = jnp.where(lax.broadcasted_iota(jnp.int32, (ROWS, LANES), 1) == me, 1.0, 0.0)
    rank_row = lax.dot_general(
        pick.astype(BF16), ranked.astype(BF16), NT, preferred_element_type=F32
    )[0:1, :]
    slot_row = lax.broadcasted_iota(jnp.int32, (slots, tokens), 0).astype(F32)
    slot_col = lax.broadcasted_iota(jnp.int32, (tokens, slots), 1).astype(F32)
    packer = jnp.where(rank_row == slot_row, 1.0, 0.0).astype(BF16)
    unpacker = jnp.where(rank_col == slot_col, 1.0, 0.0).astype(BF16)

    def got_res(k):
        t = other_tp(k)
        remote(residual, res_recv.at[t], res_ss.at[k], res_rs.at[t], me, t).wait_recv()

    loop(n_tp - 1, got_res)

    def got_proj(k):
        s, t = pair(k)
        remote(
            proj_send.at[s], proj_recv.at[t, s], proj_ss.at[k], proj_rs.at[t, s], s, t
        ).wait_recv()

    loop(n_all - 1, got_proj)
    total = proj_recv[0].astype(F32)
    for t in range(1, n_tp):
        total = total + proj_recv[t].astype(F32)
    squares = jnp.zeros((requests, LANES), F32)
    for i in range(owners):
        t, k = divmod(i, tiles)
        h = total[i] + res_recv[t, :, k * LANES : (k + 1) * LANES].astype(F32)
        hidden[t, k] = h
        squares = squares + h * h
    mean_square = jnp.sum(squares, axis=1, keepdims=True) * (1.0 / (owners * LANES))
    inv_rms = lax.rsqrt(mean_square + EPS)
    own_hidden = hidden[tp]
    normed = [
        own_hidden[k] * inv_rms * norm_gain[pl.ds(k * LANES, LANES)].astype(F32)[None]
        for k in range(tiles)
    ]
    normed = jnp.concatenate(normed, axis=0).astype(BF16)
    norm_recv[me] = normed
    start_near(norm_part)
    while left:
        left.pop(0).wait()

    finish_near(norm_part)
    got = norm_recv[...].astype(F32).reshape(owners, tiles, requests, LANES)
    rows = [got[:, k].reshape(tokens, LANES).astype(BF16) for k in range(tiles)]
    packed = jnp.dot(
        packer, jnp.concatenate(rows, axis=1), preferred_element_type=F32
    ).astype(BF16)
    for c in range(chunks):
        cols = slice(c * chunk, (c + 1) * chunk)
        both = jnp.concatenate(
            [
                jnp.dot(packed, w_gate[:, cols], preferred_element_type=F32),
                jnp.dot(packed, w_up[:, cols], preferred_element_type=F32),
            ],
            axis=1,
        )
        sums_own[c] = both
        sums_send[c] = both.astype(BF16)

        def send_sums(k):
            remote(
                sums_send.at[c],
                sums_recv.at[tp, c],
                sums_ss.at[c, k],
                sums_rs.at[c, tp],
                me,
                other_tp(k),
            ).start()

        loop(n_tp - 1, send_sums)

        def sent_sums(k, c=c):
            remote(
                sums_send.at[c],
                sums_recv.at[tp, c],
                sums_ss.at[c, k],
                sums_rs.at[c, tp],
                me,
                other_tp(k),
            ).wait_send()

        drains.append((n_tp - 1, sent_sums))
    expert_out = jnp.zeros((slots, quarter), F32)
    for c in range(chunks):
        both = sums_own[c]
        for k in range(n_tp - 1):
            t = other_tp(k)
            remote(
                sums_send.at[c], sums_recv.at[t, c], sums_ss.at[c, k], sums_rs.at[c, t], me, t
            ).wait_recv()
            both = both + sums_recv[t, c].astype(F32)
        gate, up = both[:, :chunk], both[:, chunk:]
        activated = (gate / (1.0 + jnp.exp(-gate)) * up).astype(BF16)
        expert_out = expert_out + jnp.dot(
            activated, w_down[c * chunk : (c + 1) * chunk, :], preferred_element_type=F32
        )
    spread_back = jnp.dot(unpacker, expert_out.astype(BF16), preferred_element_type=F32)
    for r in range(owners):
        part = [
            spread_back[r * requests : (r + 1) * requests, k * LANES : (k + 1) * LANES]
            for k in range(tiles)
        ]
        back_send[r] = jnp.concatenate(part, axis=0).astype(BF16)
    back_recv[me] = back_send[me]

    def send_back(k):
        p = other_owner(k)
        remote(
            back_send.at[p], back_recv.at[me], back_ss.at[k], back_rs.at[me], p, tp
        ).start()

    loop(owners - 1, send_back)

    def sent_back(k):
        p = other_owner(k)
        remote(
            back_send.at[p], back_recv.at[me], back_ss.at[k], back_rs.at[me], p, tp
        ).wait_send()

    drains.append((owners - 1, sent_back))

    def got_back(k):
        s = other_owner(k)
        remote(back_send.at[s], back_recv.at[s], back_ss.at[k], back_rs.at[s], s, tp).wait_recv()

    loop(owners - 1, got_back)
    moe = own_hidden
    for e in range(owners):
        part = back_recv[e].astype(F32).reshape(tiles, requests, LANES)
        moe = moe + part * weight_per[:, e : e + 1][None]
    for k in range(tiles):
        mixed[:, k * LANES : (k + 1) * LANES] = moe[k].astype(BF16)

    finish()


def fused_shards(n_ep, n_tp, n_sub, *args):
    owners = n_ep * n_sub
    queries, key_codes, out_weight, residual = args[0], args[3], args[10], args[11]
    norm_gain, expert_ids, capacity, w_gate, w_down = (
        args[12],
        args[13],
        args[15],
        args[16],
        args[18],
    )
    requests, heads, head_dim = queries.shape
    kv_heads = key_codes.shape[1]
    quarter, ff = residual.shape[1], w_gate.shape[2]
    tiles = quarter // LANES
    tokens = owners * requests
    slots = tokens * expert_ids.shape[1] // (2 * owners)
    chunk = 256
    chunks = ff // chunk
    group_rows = heads // kv_heads * requests
    vmem, dma = pltpu.VMEM, pltpu.SemaphoreType.DMA
    in_vmem = pl.BlockSpec(memory_space=pltpu.VMEM)
    in_smem = pl.BlockSpec(memory_space=pltpu.SMEM)
    in_any = pl.BlockSpec(memory_space=pl.ANY)
    specs = [in_vmem] * 9 + [in_smem, in_any] + [in_vmem] * 4 + [in_smem] + [in_any] * 3
    return pl.pallas_call(
        functools.partial(layer_kernel, (n_tp, n_sub, owners, slots, chunk)),
        out_shape=jax.ShapeDtypeStruct(residual.shape, BF16),
        in_specs=specs,
        out_specs=in_vmem,
        scratch_shapes=[
            vmem(out_weight.shape, BF16),
            vmem(w_gate.shape[1:], BF16),
            vmem(w_gate.shape[1:], BF16),
            vmem(w_down.shape[1:], BF16),
            vmem((kv_heads, group_rows, head_dim), F32),
            vmem((owners, kv_heads, group_rows, head_dim), BF16),
            vmem((requests, LANES), F32),
            vmem((owners, requests, LANES), F32),
            vmem((n_tp, requests, quarter), BF16),
            vmem((owners, requests, LANES), BF16),
            vmem((n_tp, owners, requests, LANES), BF16),
            vmem((n_tp, tiles, requests, LANES), F32),
            vmem((owners, tiles * requests, LANES), BF16),
            vmem((chunks, slots, 2 * chunk), F32),
            vmem((chunks, slots, 2 * chunk), BF16),
            vmem((n_tp, chunks, slots, 2 * chunk), BF16),
            vmem((owners, tiles * requests, LANES), BF16),
            vmem((owners, tiles * requests, LANES), BF16),
            dma((4,)),
            dma((kv_heads, owners)),
            dma((kv_heads, owners)),
            dma((owners,)),
            dma((owners,)),
            dma((n_tp,)),
            dma((n_tp,)),
            dma((owners * n_tp,)),
            dma((n_tp, owners)),
            dma((owners,)),
            dma((owners,)),
            dma((chunks, n_tp)),
            dma((chunks, n_tp)),
            dma((owners,)),
            dma((owners,)),
        ],
        compiler_params=pltpu.CompilerParams(collective_id=0, has_side_effects=True),
    )(*args)


def layer(n_ep, n_tp, n_sub, *args):
    requests, heads, head_dim = args[0].shape
    fits = (
        requests == ROWS
        and head_dim == LANES
        and args[3].shape[2] * 16 == LANES
        and (heads // args[3].shape[1]) % 16 == 0
        and args[10].shape[1] == LANES
        and args[11].shape[1] * n_tp == n_ep * n_sub * LANES
        and args[16].shape[0] == 1
        and n_ep * n_sub == args[15].shape[0]
        and n_ep * n_sub * requests == LANES
    )
    return fused_shards(n_ep, n_tp, n_sub, *args) if fits else shards(*args)


def solution(mesh):
    sizes = [mesh.shape[axis] for axis in ("ep", "tp", "sub")]
    return jax.shard_map(
        functools.partial(layer, *sizes),
        mesh=mesh,
        in_specs=(
            P(("groups", "ep", "sub"), "tp", None),
            P(("groups", "ep", "sub"), "tp", None),
            P(("groups", "ep", "sub"), "tp", None),
            P(("groups", "ep", "sub"), "tp", None, None),
            P(("groups", "ep", "sub"), "tp", None, None),
            P(("groups", "ep", "sub"), "tp", None, None),
            P(("groups", "ep", "sub"), "tp", None, None),
            P(("groups", "ep", "sub"), "tp", None),
            P(("groups", "ep", "sub"), "tp", None),
            P(("groups", "ep", "sub")),
            P("tp", ("ep", "sub")),
            P(("groups", "ep", "sub"), "tp"),
            P("tp"),
            P(("groups", "ep", "sub"), None),
            P(("groups", "ep", "sub"), None),
            P("groups"),
            P(("ep", "sub"), "tp", None),
            P(("ep", "sub"), "tp", None),
            P(("ep", "sub"), None, "tp"),
        ),
        out_specs=P(("groups", "ep", "sub"), "tp"),
        check_vma=False,
    )
```
